32 devices in a mesh: dp: 16 (over z, y, core), local: 2 (over x).
Axes of the slice: x: 2, y: 2, z: 4, core: 2. Of those that a mesh axis runs over, the one named last changes fastest.
Arguments:
- pre_glu: bfloat16 [32, 256, 3072], P(('dp', 'local')), may hold values from -80 to 80
- lengths: int32 [32], P(('dp', 'local')), may hold values from 1 to 256, as said below
- kernel: float32 [5, 1536], replicated, may hold values from -2.5 to 2.5
- bn_gain: float32 [1536], replicated, may hold values from 0.5 to 2
- bn_shift: float32 [1536], replicated, may hold values from -1 to 1
- w_out: bfloat16 [1536, 1536], replicated, may hold values from -0.15625 to 0.15625
- cotangent: bfloat16 [32, 256, 1536], P(('dp', 'local')), may hold values from -6 to 6
Outputs:
- grad_pre_glu: bfloat16 [32, 256, 3072], P(('dp', 'local'))
- grad_w_out: float32 [1536, 1536], P('dp', 'local')
- grad_kernel: float32 [5, 1536], replicated
- grad_gain: float32 [1536], replicated
- grad_shift: float32 [1536], replicated
The draws below stay inside these ranges and needn't reach their ends.
Inputs may be any that keep to these rules, and one draw needn't show every extreme that they name: `lengths`: each utterance's valid frames are its first ones; some utterance has all 256 frames valid.
All inputs are finite; a program needn't handle non-finite values.
Results may differ from the reference program's by a relative error of at most 0.0029.
Values sent between devices are 32-bit elements; how exact they have to be, the bound alone decides.
A program may use at most 64 MiB of HBM per device.

```python
import math
import jax
import jax.numpy as jnp
from jax import lax

WIDTH = 1536
TAPS = 5
FRAMES = 256
UTTERANCES = 32


def draw_pre_glu(key, part):
    key_a, key_b, key_c = jax.random.split(key, 3)
    ranks = jnp.arange(UTTERANCES, dtype=jnp.float32) / max(UTTERANCES - 1, 1)
    chan_scale = jnp.exp(jax.random.uniform(key_b, (2 * WIDTH,), jnp.float32, jnp.log(0.3), jnp.log(3.0)))
    offsets = 0.5 * jnp.clip(jax.random.normal(key_c, (2 * WIDTH,), jnp.float32), -4.0, 4.0)
    row_scale = 3.0 ** ranks
    base_draw = jnp.clip(jax.random.normal(key_a, (UTTERANCES, FRAMES, 2 * WIDTH), jnp.float32), -4.0, 4.0)
    values = base_draw * row_scale[:, None, None] * chan_scale + ranks[:, None, None] * offsets
    return values.astype(jnp.bfloat16)


def draw_lengths(key, part):
    ranks = jnp.arange(UTTERANCES, dtype=jnp.int32)
    floor_len = FRAMES // 3 + ranks * (FRAMES - FRAMES // 3) // max(UTTERANCES - 1, 1)
    jitter = jax.random.randint(key, (UTTERANCES,), 0, FRAMES // 8 + 1, dtype=jnp.int32)
    values = jnp.clip(floor_len - jitter, 1, FRAMES)
    return jnp.where(ranks == UTTERANCES - 1, FRAMES, values).astype(jnp.int32)


def shard_levels(stream_key, dims, pieces, smallest, high):
    def one(axis_at, shards_of):
        heights = jax.random.uniform(jax.random.fold_in(jax.random.fold_in(stream_key, 6), axis_at), (shards_of,), jnp.float32, smallest / len(pieces), high / len(pieces))
        return jnp.repeat(jnp.exp(heights), dims[axis_at] // shards_of).reshape((-1,) + (1,) * (len(dims) - axis_at - 1))

    level = one(*pieces[0])
    for cut in pieces[1:]:
        level = level * one(*cut)
    return level


def gaussian(key, extent, spread, reach, cuts=(), kind=jnp.bfloat16):
    array = spread * jax.random.normal(key, extent, jnp.float32)
    if cuts:
        array = array * shard_levels(key, extent, cuts, -0.22, 0.18)
    return jnp.clip(array, -reach, reach).astype(kind)


def setup_inputs(seed: int = 0) -> dict:
    seeds = jax.random.split(jax.random.key(seed), 8)
    return {
        "pre_glu": draw_pre_glu(jax.random.fold_in(seeds[7], 71), 0),
        "lengths": draw_lengths(jax.random.fold_in(seeds[7], 71), 0),
        "kernel": gaussian(seeds[2], (TAPS, WIDTH), TAPS ** -0.5, 2.5, (), jnp.float32),
        "bn_gain": jnp.clip(jnp.exp(jax.random.uniform(seeds[3], (WIDTH,), jnp.float32, math.log(0.5), math.log(2.0))), 0.5, 2.0),
        "bn_shift": jnp.clip(jax.random.uniform(seeds[4], (WIDTH,), jnp.float32, -1.0, 1.0), -1.0, 1.0),
        "w_out": gaussian(seeds[5], (WIDTH, WIDTH), WIDTH ** -0.5, 0.15625),
        "cotangent": gaussian(seeds[6], (UTTERANCES, FRAMES, WIDTH), 1.0, 6.0, ((0, 32),)),
    }


epsilon = 1e-05

def front_pass(pre_one, length, kernel):
    frames = pre_one.shape[0]
    model_width = kernel.shape[1]
    kernel_taps = kernel.shape[0]
    half_width = (kernel_taps - 1) // 2
    valid_mask = (jnp.arange(frames, dtype=jnp.int32)[:, None] < length).astype(jnp.float32)
    first_half = pre_one[:, :model_width].astype(jnp.float32)
    gate_value = jax.nn.sigmoid(pre_one[:, model_width:].astype(jnp.float32))
    glu_out = first_half * gate_value * valid_mask
    padded = jnp.pad(glu_out, ((half_width, half_width), (0, 0)))
    conv_out = kernel[0] * padded[0:frames]
    for j in range(1, kernel_taps):
        conv_out = conv_out + kernel[j] * padded[j:j + frames]
    return (valid_mask, first_half, gate_value, padded, conv_out)

def reference(pre_glu, lengths, kernel, bn_gain, bn_shift, w_out, cotangent):
    replicas = pre_glu.shape[0]
    frames = pre_glu.shape[1]
    model_width = kernel.shape[1]
    kernel_taps = kernel.shape[0]
    half_width = (kernel_taps - 1) // 2
    frame_total = jnp.sum(lengths).astype(jnp.float32)
    zeros_row = jnp.zeros((model_width,), jnp.float32)

    def mean_step(carry, items):
        parts = front_pass(items[0], items[1], kernel)
        return (carry + lax.optimization_barrier(jnp.sum(parts[4] * parts[0], 0)), None)
    sum_first = lax.scan(mean_step, zeros_row, (pre_glu, lengths))[0]
    mean_value = sum_first / frame_total

    def spread_step(carry, items):
        parts = front_pass(items[0], items[1], kernel)
        centered = parts[4] - mean_value
        return (carry + lax.optimization_barrier(jnp.sum(centered * centered * parts[0], 0)), None)
    sum_square = lax.scan(spread_step, zeros_row, (pre_glu, lengths))[0]
    invstd = lax.rsqrt(sum_square / frame_total + epsilon)

    def act_parts(pre_one, length, cot_one):
        parts = front_pass(pre_one, length, kernel)
        normed = (parts[4] - mean_value) * invstd
        act_in = bn_gain * normed + bn_shift
        sig_act = jax.nn.sigmoid(act_in)
        swished = (act_in * sig_act).astype(jnp.bfloat16)
        masked_cot = cot_one * parts[0].astype(jnp.bfloat16)
        grad_swish = jnp.dot(masked_cot, w_out.T, preferred_element_type=jnp.float32)
        grad_act = grad_swish * sig_act * (1.0 + act_in * (1.0 - sig_act))
        return (parts, normed, swished, masked_cot, grad_act)

    def weight_step(carry, items):
        parts, normed, swished, masked_cot, grad_act = act_parts(items[0], items[1], items[2])
        weight_sum = carry[0] + jnp.dot(swished.T, masked_cot, preferred_element_type=jnp.float32)
        return ((weight_sum, carry[1] + lax.optimization_barrier(jnp.sum(grad_act, 0)), carry[2] + lax.optimization_barrier(jnp.sum(grad_act * normed, 0))), None)
    start_carry = (jnp.zeros((model_width, model_width), jnp.float32), zeros_row, zeros_row)
    weight_sum, sum_shift, sum_gain = lax.scan(weight_step, start_carry, (pre_glu, lengths, cotangent))[0]

    def input_step(carry, items):
        parts, normed, swished, masked_cot, grad_act = act_parts(items[0], items[1], items[2])
        valid_mask, first_half, gate_value, padded = (parts[0], parts[1], parts[2], parts[3])
        grad_conv = valid_mask * bn_gain * invstd * (grad_act - (sum_shift + normed * sum_gain) / frame_total)
        kernel_part = jnp.stack([lax.optimization_barrier(jnp.sum(grad_conv * padded[j:j + frames], 0)) for j in range(kernel_taps)], 0)
        grad_padded = jnp.pad(grad_conv, ((half_width, half_width), (0, 0)))
        grad_glu = kernel[0] * grad_padded[kernel_taps - 1:kernel_taps - 1 + frames]
        for j in range(1, kernel_taps):
            grad_glu = grad_glu + kernel[j] * grad_padded[kernel_taps - 1 - j:kernel_taps - 1 - j + frames]
        grad_glu = grad_glu * valid_mask
        grad_first = grad_glu * gate_value
        grad_second = grad_glu * first_half * gate_value * (1.0 - gate_value)
        grad_pre = jnp.concatenate([grad_first, grad_second], 1).astype(jnp.bfloat16)
        return (carry + kernel_part, grad_pre)
    kernel_sum, grad_pre_glu = lax.scan(input_step, jnp.zeros((kernel_taps, model_width), jnp.float32), (pre_glu, lengths, cotangent))
    return (grad_pre_glu, weight_sum / replicas, kernel_sum / replicas, sum_gain / replicas, sum_shift / replicas)
```

```python
import functools

import jax
import jax.numpy as jnp
from jax import lax
from jax.experimental import pallas as pl
from jax.experimental.pallas import tpu as pltpu
from jax.sharding import PartitionSpec as P

epsilon = 1e-05
LANES = 128
EDGE = 8
MESH = pl.DeviceIdType.MESH
f32 = jnp.float32
bf16 = jnp.bfloat16


def split(count):
    factors = []
    while count > 1:
        wanted = (2,) if len(factors) < 2 else (4, 3, 2)
        wanted += tuple(range(2, count + 1))
        factor = next(f for f in wanted if count % f == 0)
        factors.append(factor)
        count //= factor
    return factors


class Plan:
    def __init__(self, dp, local, width, frames, taps):
        self.dp, self.local, self.width, self.frames, self.taps = dp, local, width, frames, taps
        digits, stride = [], 1
        for factor in split(dp):
            digits.append(("dp", stride, factor))
            stride *= factor
        across = ("local", 1, local)
        first, second, rest = digits[:1], digits[1:2], digits[2:]
        middle = second + ([across] if local > 1 else [])
        self.sum_groups = [g for g in [first, middle] + [[d] for d in rest] if g]
        self.rows, self.cols = width // dp, width // local
        self.chunks = self.cols // LANES
        orders = (first + middle[::-1] + rest, first + middle + rest)
        self.orders = [orders[k % 2] for k in range(self.chunks)]
        self.tiles = width // LANES
        self.up = lambda n: -(-n // 8) * 8
        self.sum_rows = [self.up(2 * self.tiles + 1), self.up(2 * self.tiles), self.up(taps * self.tiles)]

    def size(self, group):
        total = 1
        for _, _, count in group:
            total *= count
        return total

    def scratch(self):
        shapes, sems = [], 0
        for rows in self.sum_rows:
            shapes.append(pltpu.VMEM((rows, LANES), f32))
            for group in self.sum_groups:
                shapes.append(pltpu.VMEM((self.size(group), rows, LANES), f32))
                sems += self.size(group) - 1
        for order in self.orders:
            blocks = self.dp * self.local
            shapes.append(pltpu.VMEM((blocks, self.rows, LANES), f32))
            for digit in order:
                blocks //= digit[2]
                shapes.append(pltpu.VMEM((digit[2] - 1, blocks, self.rows, LANES), f32))
                sems += digit[2] - 1
        return shapes, sems


class Here:
    def __init__(self):
        self.at = {"dp": lax.axis_index("dp"), "local": lax.axis_index("local")}

    def digit(self, part):
        axis, stride, size = part
        return lax.rem(lax.div(self.at[axis], jnp.int32(stride)), jnp.int32(size))

    def index(self, group):
        total = jnp.int32(0)
        for part in group:
            total = total * part[2] + self.digit(part)
        return total

    def device(self, group, member):
        place = dict(self.at)
        for part in reversed(group):
            axis, stride, size = part
            wanted = lax.rem(member, jnp.int32(size))
            member = lax.div(member, jnp.int32(size))
            place[axis] = place[axis] + (wanted - self.digit(part)) * stride
        return (place["dp"], place["local"])


class Wire:
    def __init__(self, send, recv):
        self.send, self.recv, self.next, self.all = send, recv, 0, []

    def start(self, src, dst, device):
        copy = pltpu.make_async_remote_copy(
            src_ref=src,
            dst_ref=dst,
            send_sem=self.send.at[self.next],
            recv_sem=self.recv.at[self.next],
            device_id=device,
            device_id_type=MESH,
        )
        self.next += 1
        copy.start()
        self.all.append(copy)
        return copy


class Total:
    def __init__(self, plan, here, wire, refs):
        self.groups, self.here, self.wire = plan.sum_groups, here, wire
        self.total, self.slots = refs[0], refs[1:]
        self.copies = None
        self.size = plan.size

    def send(self, stage):
        group, slots = self.groups[stage], self.slots[stage]
        mine, count = self.here.index(group), self.size(group)
        slots[mine] = self.total[...]
        self.copies = [
            self.wire.start(
                slots.at[mine],
                slots.at[mine],
                self.here.device(group, lax.rem(mine + k, jnp.int32(count))),
            )
            for k in range(1, count)
        ]

    def take(self, stage):
        slots = self.slots[stage]
        for copy in self.copies:
            copy.wait_recv()
        value = slots[0]
        for k in range(1, self.size(self.groups[stage])):
            value = value + slots[k]
        self.total[...] = value


class Scatter:
    def __init__(self, order, here, wire, refs):
        self.order, self.here, self.wire = order, here, wire
        self.held, self.landing = [refs[0]], refs[1:]
        self.held += [slot.at[0] for slot in self.landing]
        self.copies = None

    def send(self, stage):
        digit, landing = self.order[stage], self.landing[stage]
        mine, count, blocks = self.here.digit(digit), digit[2], landing.shape[1]
        self.copies = []
        for k in range(1, count):
            member = lax.rem(mine + k, jnp.int32(count))
            self.copies.append(
                self.wire.start(
                    self.held[stage].at[pl.ds(member * blocks, blocks)],
                    landing.at[k - 1],
                    self.here.device([digit], member),
                )
            )

    def take(self, stage):
        digit, landing, held = self.order[stage], self.landing[stage], self.held[stage]
        mine, count, blocks = self.here.digit(digit), digit[2], landing.shape[1]
        for copy in self.copies:
            copy.wait_recv()

        def add(b, carry):
            value = held[mine * blocks + b]
            for k in range(count - 1):
                value = value + landing[k, b]
            landing[0, b] = value
            return carry

        lax.fori_loop(0, blocks, add, 0)


def module_kernel(plan, count_sems, *refs):
    (length_ref, pre_ref, taps_ref, gain_ref, shift_ref, w_hbm, cot_hbm) = refs[:7]
    (pre_out, weight_out, taps_out, gain_out, shift_out) = refs[7:12]
    (w_ref, cot_ref, glu, conv, swish_t, arriving, conv_grad, pre_grad, local_sems, send, recv) = refs[12:23]
    pool = list(refs[23:])
    frames, width, taps, tiles = plan.frames, plan.width, plan.taps, plan.tiles
    half = (taps - 1) // 2
    here, wire = Here(), Wire(send, recv)

    w_copy = pltpu.make_async_copy(w_hbm, w_ref, local_sems.at[0])
    cot_copy = pltpu.make_async_copy(cot_hbm.at[0], cot_ref, local_sems.at[1])
    cot_copy.start()
    w_copy.start()

    barrier = pltpu.get_barrier_semaphore()
    peers = 0
    for group in plan.sum_groups:
        for k in range(1, plan.size(group)):
            member = lax.rem(here.index(group) + k, jnp.int32(plan.size(group)))
            pl.semaphore_signal(barrier, inc=1, device_id=here.device(group, member), device_id_type=MESH)
            peers += 1

    totals = []
    for _ in plan.sum_rows:
        take = 1 + len(plan.sum_groups)
        totals.append(Total(plan, here, wire, pool[:take]))
        pool = pool[take:]
    scatters = []
    for order in plan.orders:
        take = 1 + len(order)
        scatters.append(Scatter(order, here, wire, pool[:take]))
        pool = pool[take:]

    length = length_ref[0]
    rows_at = lax.broadcasted_iota(jnp.int32, (frames, LANES), 0)

    def valid():
        return jnp.where(rows_at < length, jnp.float32(1), jnp.float32(0))

    def at(tile, base=0):
        return pl.ds(pl.multiple_of(base + tile * LANES, LANES), LANES)

    def row(ref, r):
        return ref[pl.ds(r, 1), :]

    def column_sum(value):
        return jnp.sum(value, 0, keepdims=True)

    for ref in (glu, conv_grad):
        ref[0:EDGE, :] = jnp.zeros((EDGE, width), f32)
        ref[EDGE + frames :, :] = jnp.zeros((EDGE, width), f32)
    for total in totals:
        total.total[...] = jnp.zeros(total.total.shape, f32)

    stats = totals[0].total

    def front(tile, carry):
        cols = at(tile)
        mask = valid()
        first = pre_ref[0, :, cols].astype(f32)
        gate = jax.nn.sigmoid(pre_ref[0, :, at(tile, width)].astype(f32))
        glu[EDGE : EDGE + frames, cols] = first * gate * mask
        out = taps_ref[0:1, cols] * glu[EDGE - half : EDGE - half + frames, cols]
        for j in range(1, taps):
            start = EDGE + j - half
            out = out + taps_ref[j : j + 1, cols] * glu[start : start + frames, cols]
        conv[:, cols] = out
        kept = out * mask
        stats[pl.ds(tile, 1), :] = column_sum(kept)
        stats[pl.ds(tiles + tile, 1), :] = column_sum(out * kept)
        return carry

    lax.fori_loop(0, tiles, front, 0)
    stats[2 * tiles : 2 * tiles + 1, :] = jnp.full((1, LANES), length, jnp.int32).astype(f32)

    pl.semaphore_wait(barrier, peers)
    stages = len(plan.sum_groups)
    totals[0].send(0)
    cot_copy.wait()

    def mask_cot(tile, carry):
        cols = at(tile)
        cot_ref[:, cols] = (cot_ref[:, cols].astype(f32) * valid()).astype(bf16)
        return carry

    lax.fori_loop(0, tiles, mask_cot, 0)
    totals[0].take(0)
    totals[0].send(1)
    w_copy.wait()

    wide = 2 * LANES if tiles % 2 == 0 else LANES

    def back_matmul(tile, carry):
        cols = pl.ds(pl.multiple_of(tile * wide, wide), wide)
        arriving[:, cols] = lax.dot_general(
            cot_ref[...], w_ref[cols, :], (((1,), (1,)), ((), ())), preferred_element_type=f32
        )
        return carry

    lax.fori_loop(0, width // wide, back_matmul, 0)
    totals[0].take(1)
    for stage in range(2, stages):
        totals[0].send(stage)
        totals[0].take(stage)

    def moments(tile):
        count = row(stats, 2 * tiles)
        mean = row(stats, tile) / count
        variance = row(stats, tiles + tile) / count - mean * mean
        return count, mean, lax.rsqrt(variance + epsilon)

    sums = totals[1].total

    def activate(tile, carry):
        cols = at(tile)
        _, mean, invstd = moments(tile)
        normed = (conv[:, cols] - mean) * invstd
        act = gain_ref[0:1, cols] * normed + shift_ref[0:1, cols]
        sig = jax.nn.sigmoid(act)
        swish_t[cols, :] = (act * sig).T.astype(bf16)
        grad = arriving[:, cols] * sig * (1.0 + act * (1.0 - sig))
        arriving[:, cols] = grad
        sums[pl.ds(tile, 1), :] = column_sum(grad)
        sums[pl.ds(tiles + tile, 1), :] = column_sum(grad * normed)
        return carry

    lax.fori_loop(0, tiles, activate, 0)
    totals[1].send(0)

    def weight_chunk(k):
        scatter = scatters[k]
        parts = [
            cot_ref[:, c * plan.cols + k * LANES : c * plan.cols + (k + 1) * LANES]
            for c in range(plan.local)
        ]
        product = jnp.dot(swish_t[...], jnp.concatenate(parts, 1), preferred_element_type=f32)
        for d in range(plan.dp):
            for c in range(plan.local):
                block = 0
                for axis, stride, size in scatter.order:
                    block = block * size + ((d if axis == "dp" else c) // stride) % size
                scatter.held[0][block] = product[
                    d * plan.rows : (d + 1) * plan.rows, c * LANES : (c + 1) * LANES
                ]
        scatter.send(0)

    chunks = plan.chunks
    steps = len(plan.orders[0])
    for k in range(min(2, chunks)):
        weight_chunk(k)
    totals[1].take(0)
    totals[1].send(1)
    for k in range(min(2, chunks)):
        scatters[k].take(0)
        scatters[k].send(1)
    for k in range(2, chunks):
        weight_chunk(k)
    totals[1].take(1)
    for stage in range(2, stages):
        totals[1].send(stage)
        if stage == 2:
            for k in range(2, chunks):
                scatters[k].take(0)
                scatters[k].send(1)
        totals[1].take(stage)

    kernel_sums = totals[2].total

    def finish(tile, carry):
        cols = at(tile)
        mask = valid()
        count, mean, invstd = moments(tile)
        normed = (conv[:, cols] - mean) * invstd
        grad = (
            mask
            * (gain_ref[0:1, cols] * invstd)
            * (arriving[:, cols] - (row(sums, tile) + normed * row(sums, tiles + tile)) / count)
        )
        conv_grad[EDGE : EDGE + frames, cols] = grad
        back = jnp.zeros((frames, LANES), f32)
        for j in range(taps):
            start = EDGE + j - half
            kernel_sums[pl.ds(j * tiles + tile, 1), :] = column_sum(
                grad * glu[start : start + frames, cols]
            )
            start = EDGE + half - j
            back = back + taps_ref[j : j + 1, cols] * conv_grad[start : start + frames, cols]
        first = pre_ref[0, :, cols].astype(f32)
        gate = jax.nn.sigmoid(pre_ref[0, :, at(tile, width)].astype(f32))
        back = back * mask * gate
        pre_grad[:, cols] = back.astype(bf16)
        pre_grad[:, at(tile, width)] = (back * first * (1.0 - gate)).astype(bf16)
        return carry

    lax.fori_loop(0, tiles, finish, 0)
    out_copy = pltpu.make_async_copy(pre_grad, pre_out.at[0], local_sems.at[2])
    out_copy.start()
    replicas = plan.dp * plan.local
    totals[2].send(0)
    for t in range(tiles):
        cols = slice(t * LANES, (t + 1) * LANES)
        shift_out[0:1, cols] = sums[t : t + 1, :] / replicas
        gain_out[0:1, cols] = sums[tiles + t : tiles + t + 1, :] / replicas
    totals[2].take(0)
    totals[2].send(1)
    for k in range(chunks):
        scatters[k].take(1)
        scatters[k].send(2)
    totals[2].take(1)
    for stage in range(2, stages):
        totals[2].send(stage)
        for k in range(chunks):
            if stage + 1 < steps:
                scatters[k].take(stage)
                scatters[k].send(stage + 1)
        totals[2].take(stage)
    for t in range(tiles):
        cols = slice(t * LANES, (t + 1) * LANES)
        for j in range(taps):
            at_row = j * tiles + t
            taps_out[j : j + 1, cols] = kernel_sums[at_row : at_row + 1, :] / replicas
    for k in range(chunks):
        scatters[k].take(steps - 1)
        weight_out[:, k * LANES : (k + 1) * LANES] = scatters[k].landing[steps - 1][0, 0] / replicas
    for copy in wire.all:
        copy.wait_send()
    out_copy.wait()


def on_device(pre_glu, lengths, kernel, bn_gain, bn_shift, w_out, cotangent):
    frames, taps, width = pre_glu.shape[1], kernel.shape[0], kernel.shape[1]
    plan = Plan(lax.axis_size("dp"), lax.axis_size("local"), width, frames, taps)
    pool, sems = plan.scratch()
    vmem, anywhere = pl.BlockSpec(memory_space=pltpu.VMEM), pl.BlockSpec(memory_space=pl.ANY)
    smem = pl.BlockSpec(memory_space=pltpu.SMEM)
    grad_pre, weight, kernel_grad, gain_grad, shift_grad = pl.pallas_call(
        functools.partial(module_kernel, plan, sems),
        out_shape=(
            jax.ShapeDtypeStruct(pre_glu.shape, bf16),
            jax.ShapeDtypeStruct((plan.rows, plan.cols), f32),
            jax.ShapeDtypeStruct((taps, width), f32),
            jax.ShapeDtypeStruct((1, width), f32),
            jax.ShapeDtypeStruct((1, width), f32),
        ),
        in_specs=[smem, vmem, vmem, vmem, vmem, anywhere, anywhere],
        out_specs=(anywhere, vmem, vmem, vmem, vmem),
        scratch_shapes=[
            pltpu.VMEM((width, width), bf16),
            pltpu.VMEM((frames, width), bf16),
            pltpu.VMEM((frames + 2 * EDGE, width), f32),
            pltpu.VMEM((frames, width), f32),
            pltpu.VMEM((width, frames), bf16),
            pltpu.VMEM((frames, width), f32),
            pltpu.VMEM((frames + 2 * EDGE, width), f32),
            pltpu.VMEM((frames, 2 * width), bf16),
            pltpu.SemaphoreType.DMA((3,)),
            pltpu.SemaphoreType.DMA((sems,)),
            pltpu.SemaphoreType.DMA((sems,)),
        ]
        + pool,
        compiler_params=pltpu.CompilerParams(
            collective_id=0, has_side_effects=True, vmem_limit_bytes=60 * 1024 * 1024
        ),
    )(lengths, pre_glu, kernel, bn_gain[None], bn_shift[None], w_out, cotangent)
    return grad_pre, weight, kernel_grad, gain_grad[0], shift_grad[0]


def solution(mesh):
    return jax.shard_map(
        on_device,
        mesh=mesh,
        in_specs=(
            P(("dp", "local"), None, None),
            P(("dp", "local")),
            P(),
            P(),
            P(),
            P(),
            P(("dp", "local"), None, None),
        ),
        out_specs=(P(("dp", "local"), None, None), P("dp", "local"), P(), P(), P()),
        check_vma=False,
    )
```

```python
import functools

import jax
import jax.numpy as jnp
from jax import lax
from jax.experimental import pallas as pl
from jax.experimental.pallas import tpu as pltpu
from jax.sharding import PartitionSpec as P

epsilon = 1e-05
LANES = 128
EDGE = 8
MESH = pl.DeviceIdType.MESH
f32 = jnp.float32
bf16 = jnp.bfloat16


def split(count):
    factors = []
    while count > 1:
        wanted = (2,) if len(factors) < 2 else (4, 3, 2)
        wanted += tuple(range(2, count + 1))
        factor = next(f for f in wanted if count % f == 0)
        factors.append(factor)
        count //= factor
    return factors


class Plan:
    def __init__(self, dp, local, width, frames, taps):
        self.dp, self.local, self.width, self.frames, self.taps = dp, local, width, frames, taps
        digits, stride = [], 1
        for factor in split(dp):
            digits.append(("dp", stride, factor))
            stride *= factor
        across = ("local", 1, local)
        first, second, rest = digits[:1], digits[1:2], digits[2:]
        middle = second + ([across] if local > 1 else [])
        self.sum_groups = [g for g in [first, middle] + [[d] for d in rest] if g]
        self.rows, self.cols = width // dp, width // local
        self.chunks = self.cols // LANES
        early = (first + middle[1:] + rest + middle[:1], first + middle[:1] + rest + middle[1:])
        late = (first + middle[::-1] + rest, first + middle + rest)
        self.halves = 2 if self.rows % 16 == 0 else 1
        self.part = self.rows // self.halves
        self.pieces, self.orders, self.jobs = {}, [], []
        for low in range(0, self.chunks, 2):
            for part in range(self.halves):
                job = []
                for chunk in range(low, min(low + 2, self.chunks)):
                    job.append(len(self.orders))
                    self.pieces[chunk, part] = len(self.orders)
                    self.orders.append((early if low == 0 else late)[chunk % 2])
                self.jobs.append(job)
        self.tiles = width // LANES
        self.up = lambda n: -(-n // 8) * 8
        self.sum_rows = [self.up(2 * self.tiles + 1), self.up(2 * self.tiles), self.up(taps * self.tiles)]

    def size(self, group):
        total = 1
        for _, _, count in group:
            total *= count
        return total

    def scratch(self):
        shapes, sems = [], 0
        for rows in self.sum_rows:
            shapes.append(pltpu.VMEM((rows, LANES), f32))
            for group in self.sum_groups:
                shapes.append(pltpu.VMEM((self.size(group), rows, LANES), f32))
                sems += self.size(group) - 1
        for order in self.orders:
            blocks = self.dp * self.local
            shapes.append(pltpu.VMEM((blocks, self.part, LANES), f32))
            for digit in order:
                blocks //= digit[2]
                shapes.append(pltpu.VMEM((digit[2] - 1, blocks, self.part, LANES), f32))
                sems += digit[2] - 1
        return shapes, sems


class Here:
    def __init__(self):
        self.at = {"dp": lax.axis_index("dp"), "local": lax.axis_index("local")}

    def digit(self, part):
        axis, stride, size = part
        return lax.rem(lax.div(self.at[axis], jnp.int32(stride)), jnp.int32(size))

    def index(self, group):
        total = jnp.int32(0)
        for part in group:
            total = total * part[2] + self.digit(part)
        return total

    def device(self, group, member):
        place = dict(self.at)
        for part in reversed(group):
            axis, stride, size = part
            wanted = lax.rem(member, jnp.int32(size))
            member = lax.div(member, jnp.int32(size))
            place[axis] = place[axis] + (wanted - self.digit(part)) * stride
        return (place["dp"], place["local"])


class Wire:
    def __init__(self, send, recv):
        self.send, self.recv, self.next, self.all = send, recv, 0, []

    def start(self, src, dst, device):
        copy = pltpu.make_async_remote_copy(
            src_ref=src,
            dst_ref=dst,
            send_sem=self.send.at[self.next],
            recv_sem=self.recv.at[self.next],
            device_id=device,
            device_id_type=MESH,
        )
        self.next += 1
        copy.start()
        self.all.append(copy)
        return copy


class Total:
    def __init__(self, plan, here, wire, refs):
        self.groups, self.here, self.wire = plan.sum_groups, here, wire
        self.total, self.slots = refs[0], refs[1:]
        self.copies, self.stage = None, -1
        self.size = plan.size

    def send(self, stage):
        group, slots = self.groups[stage], self.slots[stage]
        mine, count = self.here.index(group), self.size(group)
        slots[mine] = self.total[...]
        self.copies = [
            self.wire.start(
                slots.at[mine],
                slots.at[mine],
                self.here.device(group, lax.rem(mine + k, jnp.int32(count))),
            )
            for k in range(1, count)
        ]

    def take(self, stage):
        slots = self.slots[stage]
        for copy in self.copies:
            copy.wait_recv()
        value = slots[0]
        for k in range(1, self.size(self.groups[stage])):
            value = value + slots[k]
        self.total[...] = value

    def advance(self):
        if self.stage == len(self.groups):
            return False
        if self.stage >= 0:
            self.take(self.stage)
        self.stage += 1
        if self.stage < len(self.groups):
            self.send(self.stage)
        return True


class Scatter:
    def __init__(self, order, here, wire, refs):
        self.order, self.here, self.wire = order, here, wire
        self.held, self.landing = [refs[0]], refs[1:]
        self.held += [slot.at[0] for slot in self.landing]
        self.copies, self.stage = None, -1

    def advance(self):
        if self.stage == len(self.order):
            return False
        if self.stage >= 0:
            self.take(self.stage)
        self.stage += 1
        if self.stage < len(self.order):
            self.send(self.stage)
        return True

    def send(self, stage):
        digit, landing = self.order[stage], self.landing[stage]
        mine, count, blocks = self.here.digit(digit), digit[2], landing.shape[1]
        self.copies = []
        for k in range(1, count):
            member = lax.rem(mine + k, jnp.int32(count))
            self.copies.append(
                self.wire.start(
                    self.held[stage].at[pl.ds(member * blocks, blocks)],
                    landing.at[k - 1],
                    self.here.device([digit], member),
                )
            )

    def take(self, stage):
        digit, landing, held = self.order[stage], self.landing[stage], self.held[stage]
        mine, count, blocks = self.here.digit(digit), digit[2], landing.shape[1]
        for copy in self.copies:
            copy.wait_recv()

        def add(b, carry):
            value = held[mine * blocks + b]
            for k in range(count - 1):
                value = value + landing[k, b]
            landing[0, b] = value
            return carry

        lax.fori_loop(0, blocks, add, 0)


def module_kernel(plan, count_sems, *refs):
    (length_ref, pre_ref, taps_ref, gain_ref, shift_ref, w_hbm, cot_hbm) = refs[:7]
    (pre_out, weight_out, taps_out, gain_out, shift_out) = refs[7:12]
    (w_ref, cot_ref, glu, conv, swish_t, arriving, conv_grad, pre_grad, local_sems, send, recv) = refs[12:23]
    pool = list(refs[23:])
    frames, width, taps, tiles = plan.frames, plan.width, plan.taps, plan.tiles
    half = (taps - 1) // 2
    here, wire = Here(), Wire(send, recv)

    w_copy = pltpu.make_async_copy(w_hbm, w_ref, local_sems.at[0])
    cot_copy = pltpu.make_async_copy(cot_hbm.at[0], cot_ref, local_sems.at[1])
    cot_copy.start()
    w_copy.start()

    barrier = pltpu.get_barrier_semaphore()
    peers = 0
    for group in plan.sum_groups:
        for k in range(1, plan.size(group)):
            member = lax.rem(here.index(group) + k, jnp.int32(plan.size(group)))
            pl.semaphore_signal(barrier, inc=1, device_id=here.device(group, member), device_id_type=MESH)
            peers += 1

    totals = []
    for _ in plan.sum_rows:
        take = 1 + len(plan.sum_groups)
        totals.append(Total(plan, here, wire, pool[:take]))
        pool = pool[take:]
    scatters = []
    for order in plan.orders:
        take = 1 + len(order)
        scatters.append(Scatter(order, here, wire, pool[:take]))
        pool = pool[take:]

    length = length_ref[0]
    rows_at = lax.broadcasted_iota(jnp.int32, (frames, LANES), 0)

    def valid():
        return jnp.where(rows_at < length, jnp.float32(1), jnp.float32(0))

    def at(tile, base=0):
        return pl.ds(pl.multiple_of(base + tile * LANES, LANES), LANES)

    def row(ref, r):
        return ref[pl.ds(r, 1), :]

    def wide_row(ref, tile):
        return ref[at(tile)].reshape(1, LANES)

    def column_sum(value):
        return jnp.sum(value, 0, keepdims=True)

    for ref in (glu, conv_grad):
        ref[0:EDGE, :] = jnp.zeros((EDGE, width), f32)
        ref[EDGE + frames :, :] = jnp.zeros((EDGE, width), f32)
    for total in totals:
        total.total[...] = jnp.zeros(total.total.shape, f32)

    stats = totals[0].total

    def front(tile, carry):
        cols = at(tile)
        mask = valid()
        first = pre_ref[0, :, cols].astype(f32)
        gate = jax.nn.sigmoid(pre_ref[0, :, at(tile, width)].astype(f32))
        glu[EDGE : EDGE + frames, cols] = first * gate * mask
        out = taps_ref[0:1, cols] * glu[EDGE - half : EDGE - half + frames, cols]
        for j in range(1, taps):
            start = EDGE + j - half
            out = out + taps_ref[j : j + 1, cols] * glu[start : start + frames, cols]
        conv[:, cols] = out
        kept = out * mask
        stats[pl.ds(tile, 1), :] = column_sum(kept)
        stats[pl.ds(tiles + tile, 1), :] = column_sum(out * kept)
        return carry

    lax.fori_loop(0, tiles, front, 0)
    stats[2 * tiles : 2 * tiles + 1, :] = jnp.full((1, LANES), length, jnp.int32).astype(f32)

    pl.semaphore_wait(barrier, peers)
    totals[0].advance()
    cot_copy.wait()

    def mask_cot(tile, carry):
        cols = at(tile)
        cot_ref[:, cols] = (cot_ref[:, cols].astype(f32) * valid()).astype(bf16)
        return carry

    lax.fori_loop(0, tiles, mask_cot, 0)
    totals[0].advance()
    w_copy.wait()

    wide = 2 * LANES if tiles % 2 == 0 else LANES

    def back_matmul(tile, carry):
        cols = pl.ds(pl.multiple_of(tile * wide, wide), wide)
        arriving[:, cols] = lax.dot_general(
            cot_ref[...], w_ref[cols, :], (((1,), (1,)), ((), ())), preferred_element_type=f32
        )
        return carry

    lax.fori_loop(0, width // wide, back_matmul, 0)
    while totals[0].advance():
        pass

    def moments(tile):
        count = row(stats, 2 * tiles)
        mean = row(stats, tile) / count
        variance = row(stats, tiles + tile) / count - mean * mean
        return count, mean, lax.rsqrt(variance + epsilon)

    sums = totals[1].total

    def normed_act(tile):
        cols = at(tile)
        _, mean, invstd = moments(tile)
        normed = (conv[:, cols] - mean) * invstd
        act = wide_row(gain_ref, tile) * normed + wide_row(shift_ref, tile)
        return normed, act, jax.nn.sigmoid(act)

    def activate(tile, carry):
        _, act, sig = normed_act(tile)
        swish_t[at(tile), :] = (act * sig).T.astype(bf16)
        return carry

    def act_grad(tile, carry):
        cols = at(tile)
        normed, act, sig = normed_act(tile)
        grad = arriving[:, cols] * sig * (1.0 + act * (1.0 - sig))
        arriving[:, cols] = grad
        sums[pl.ds(tile, 1), :] = column_sum(grad)
        sums[pl.ds(tiles + tile, 1), :] = column_sum(grad * normed)
        return carry

    def weight_chunk(k):
        if k >= plan.chunks:
            return
        parts = [
            cot_ref[:, c * plan.cols + k * LANES : c * plan.cols + (k + 1) * LANES]
            for c in range(plan.local)
        ]
        product = jnp.dot(swish_t[...], jnp.concatenate(parts, 1), preferred_element_type=f32)
        for part in range(plan.halves):
            scatter = scatters[plan.pieces[k, part]]
            for d in range(plan.dp):
                for c in range(plan.local):
                    block = 0
                    for axis, stride, size in scatter.order:
                        block = block * size + ((d if axis == "dp" else c) // stride) % size
                    low = d * plan.rows + part * plan.part
                    scatter.held[0][block] = product[
                        low : low + plan.part, c * LANES : (c + 1) * LANES
                    ]
            scatter.advance()

    def go(*jobs):
        for job in jobs:
            if job < len(plan.jobs):
                for piece in plan.jobs[job]:
                    scatters[piece].advance()

    lax.fori_loop(0, tiles, activate, 0)
    weight_chunk(0)
    weight_chunk(1)
    lax.fori_loop(0, tiles, act_grad, 0)
    totals[1].advance()
    go(0)
    totals[1].advance()
    go(1)
    weight_chunk(2)
    weight_chunk(3)
    totals[1].advance()
    go(0)
    weight_chunk(4)
    weight_chunk(5)
    for k in range(6, plan.chunks):
        weight_chunk(k)
    go(2, 3)
    while totals[1].advance():
        pass

    kernel_sums = totals[2].total

    def finish(tile, carry):
        cols = at(tile)
        mask = valid()
        count, mean, invstd = moments(tile)
        normed = (conv[:, cols] - mean) * invstd
        grad = (
            mask
            * (wide_row(gain_ref, tile) * invstd)
            * (arriving[:, cols] - (row(sums, tile) + normed * row(sums, tiles + tile)) / count)
        )
        conv_grad[EDGE : EDGE + frames, cols] = grad
        back = jnp.zeros((frames, LANES), f32)
        for j in range(taps):
            start = EDGE + j - half
            kernel_sums[pl.ds(j * tiles + tile, 1), :] = column_sum(
                grad * glu[start : start + frames, cols]
            )
            start = EDGE + half - j
            back = back + taps_ref[j : j + 1, cols] * conv_grad[start : start + frames, cols]
        first = pre_ref[0, :, cols].astype(f32)
        gate = jax.nn.sigmoid(pre_ref[0, :, at(tile, width)].astype(f32))
        back = back * mask * gate
        pre_grad[:, cols] = back.astype(bf16)
        pre_grad[:, at(tile, width)] = (back * first * (1.0 - gate)).astype(bf16)
        return carry

    lax.fori_loop(0, tiles, finish, 0)
    out_copy = pltpu.make_async_copy(pre_grad, pre_out.at[0], local_sems.at[2])
    out_copy.start()
    replicas = plan.dp * plan.local
    totals[2].advance()
    go(1, 4)
    totals[2].advance()
    for t in range(tiles):
        cols = slice(t * LANES, (t + 1) * LANES)
        shift_out[cols] = (sums[t : t + 1, :] / replicas).reshape(LANES)
        gain_out[cols] = (sums[tiles + t : tiles + t + 1, :] / replicas).reshape(LANES)
    go(2, 3, 5, 0, 2)
    totals[2].advance()
    go(1, 3, 4, 5, 4, 5)
    while totals[2].advance():
        pass
    for t in range(tiles):
        cols = slice(t * LANES, (t + 1) * LANES)
        for j in range(taps):
            at_row = j * tiles + t
            taps_out[j : j + 1, cols] = kernel_sums[at_row : at_row + 1, :] / replicas
    while any([scatter.advance() for scatter in scatters]):
        pass
    for (chunk, part), piece in plan.pieces.items():
        weight_out[
            part * plan.part : (part + 1) * plan.part, chunk * LANES : (chunk + 1) * LANES
        ] = scatters[piece].landing[-1][0, 0] / replicas
    for copy in wire.all:
        copy.wait_send()
    out_copy.wait()


def on_device(pre_glu, lengths, kernel, bn_gain, bn_shift, w_out, cotangent):
    frames, taps, width = pre_glu.shape[1], kernel.shape[0], kernel.shape[1]
    plan = Plan(lax.axis_size("dp"), lax.axis_size("local"), width, frames, taps)
    pool, sems = plan.scratch()
    vmem, anywhere = pl.BlockSpec(memory_space=pltpu.VMEM), pl.BlockSpec(memory_space=pl.ANY)
    smem = pl.BlockSpec(memory_space=pltpu.SMEM)
    grad_pre, weight, kernel_grad, gain_grad, shift_grad = pl.pallas_call(
        functools.partial(module_kernel, plan, sems),
        out_shape=(
            jax.ShapeDtypeStruct(pre_glu.shape, bf16),
            jax.ShapeDtypeStruct((plan.rows, plan.cols), f32),
            jax.ShapeDtypeStruct((taps, width), f32),
            jax.ShapeDtypeStruct((width,), f32),
            jax.ShapeDtypeStruct((width,), f32),
        ),
        in_specs=[smem, vmem, vmem, vmem, vmem, anywhere, anywhere],
        out_specs=(anywhere, vmem, vmem, vmem, vmem),
        scratch_shapes=[
            pltpu.VMEM((width, width), bf16),
            pltpu.VMEM((frames, width), bf16),
            pltpu.VMEM((frames + 2 * EDGE, width), f32),
            pltpu.VMEM((frames, width), f32),
            pltpu.VMEM((width, frames), bf16),
            pltpu.VMEM((frames, width), f32),
            pltpu.VMEM((frames + 2 * EDGE, width), f32),
            pltpu.VMEM((frames, 2 * width), bf16),
            pltpu.SemaphoreType.DMA((3,)),
            pltpu.SemaphoreType.DMA((sems,)),
            pltpu.SemaphoreType.DMA((sems,)),
        ]
        + pool,
        compiler_params=pltpu.CompilerParams(
            collective_id=0, has_side_effects=True, vmem_limit_bytes=60 * 1024 * 1024
        ),
    )(lengths, pre_glu, kernel, bn_gain, bn_shift, w_out, cotangent)
    return grad_pre, weight, kernel_grad, gain_grad, shift_grad


def solution(mesh):
    return jax.shard_map(
        on_device,
        mesh=mesh,
        in_specs=(
            P(("dp", "local"), None, None),
            P(("dp", "local")),
            P(),
            P(),
            P(),
            P(),
            P(("dp", "local"), None, None),
        ),
        out_specs=(P(("dp", "local"), None, None), P("dp", "local"), P(), P(), P()),
        check_vma=False,
    )
```
